32 devices in a mesh: gx: 4 (over y, x), gy: 4 (over z), gz: 2 (over core).
Axes of the slice: x: 2, y: 2, z: 4, core: 2. Of those that a mesh axis runs over, the one named last changes fastest.
Arguments:
- estimate: float32 [16, 256, 512], P('gz', 'gx', 'gy'), may hold values from 0.25 to 4
- view_data: float32 [16, 256, 512], P('gz', 'gx', 'gy'), may hold values from 0.25 to 4
- psf_stack: float32 [6, 31, 31, 31], replicated, may hold values from 0.01 to 1.53, as said below
- view_index: int32 [1], replicated, may hold values from 0 to 5
Outputs:
- updated_estimate: float32 [16, 256, 512], P('gz', 'gx', 'gy')
- level_one: float32 [8, 128, 256], P('gz', 'gx', 'gy')
- level_two: float32 [4, 64, 128], P('gz', 'gx', 'gy')
- level_three: float32 [2, 32, 64], P('gz', 'gx', 'gy')
- level_four: float32 [1, 16, 32], P(None, 'gx', 'gy')
- level_five: float32 [1, 8, 16], replicated
The draws below stay inside these ranges and needn't reach their ends.
Inputs may be any that keep to these rules, and one draw needn't show every extreme that they name: `psf_stack`: every entry of every view's point spread function is positive.
All inputs are finite; a program needn't handle non-finite values.
Results may differ from the reference program's by a relative error of at most 0.000075.
Values sent between devices are 32-bit elements; how exact they have to be, the bound alone decides.
A program may use at most 128 MiB of HBM per device.

```python
import math
import jax
import jax.numpy as jnp
from jax import lax

HALO = 15
VIEWS = 6
NX = 256
NY = 512
NZ = 16


def draw_psf_stack(key, part):
    extent = 2 * HALO + 1
    first, second, third = jax.random.split(jax.random.fold_in(key, 7), 3)
    widths = jax.random.uniform(first, (VIEWS, 3), jnp.float32, 1.0, 4.5)
    offsets = jnp.arange(extent, dtype=jnp.float32) - HALO
    depth_term = offsets[None, :, None, None] / widths[:, 0, None, None, None]
    row_term = offsets[None, None, :, None] / widths[:, 1, None, None, None]
    column_term = offsets[None, None, None, :] / widths[:, 2, None, None, None]
    exponent = depth_term * depth_term + row_term * row_term + column_term * column_term
    roughness = jax.random.uniform(second, (VIEWS, extent, extent, extent), jnp.float32, 0.5, 1.5)
    floor_part = 0.02 * jax.random.uniform(third, (VIEWS, extent, extent, extent), jnp.float32, 0.5, 1.5)
    return jnp.exp(-0.5 * exponent) * roughness + floor_part


def levels(own_key, shape, cuts, least, high):
    def one(position, parts):
        steps = jax.random.uniform(jax.random.fold_in(jax.random.fold_in(own_key, 6), position), (parts,), jnp.float32, least / len(cuts), high / len(cuts))
        return jnp.repeat(jnp.exp(steps), shape[position] // parts).reshape((-1,) + (1,) * (len(shape) - position - 1))

    loudness = one(*cuts[0])
    for cut in cuts[1:]:
        loudness = loudness * one(*cut)
    return loudness


def setup_inputs(seed: int = 0) -> dict:
    streams_of = jax.random.split(jax.random.key(seed), 5)
    return {
        "estimate": jnp.clip(jnp.exp(math.log(4.0) - 2.7725887 * jax.random.uniform(streams_of[0], (NZ, NX, NY), jnp.float32) ** levels(streams_of[0], (NZ, NX, NY), ((0, 2), (1, 4), (2, 4)), -0.2, 0.2)), 0.25, 4.0),
        "view_data": jnp.clip(jnp.exp(math.log(4.0) - 2.7725887 * jax.random.uniform(streams_of[1], (NZ, NX, NY), jnp.float32) ** levels(streams_of[1], (NZ, NX, NY), ((0, 2), (1, 4), (2, 4)), -0.2, 0.2)), 0.25, 4.0),
        "psf_stack": draw_psf_stack(jax.random.fold_in(streams_of[4], 71), 0),
        "view_index": jax.random.randint(streams_of[3], (1,), 0, VIEWS).astype(jnp.int32),
    }


def convolve(volume, kernel):
    radius = (kernel.shape[0] - 1) // 2
    fft_sizes = tuple(((extent + 2 * radius + 15) // 16) * 16 for extent in volume.shape)
    product = jnp.fft.rfftn(volume, fft_sizes) * jnp.fft.rfftn(kernel, fft_sizes)
    full_conv = jnp.fft.irfftn(product, fft_sizes)
    plane_count, row_count, column_count = volume.shape
    return full_conv[radius:radius + plane_count, radius:radius + row_count, radius:radius + column_count].astype(jnp.float32)


def average_blocks(volume, depth):
    plane_count, row_count, column_count = volume.shape
    if depth:
        blocks = volume.reshape(plane_count // 2, 2, row_count // 2, 2, column_count // 2, 2)
        return jnp.mean(blocks, axis=(1, 3, 5))
    blocks = volume.reshape(plane_count, row_count // 2, 2, column_count // 2, 2)
    return jnp.mean(blocks, axis=(2, 4))


def reference(estimate, view_data, psf_stack, view_index):
    kernel = lax.dynamic_index_in_dim(psf_stack, view_index[0], 0, keepdims=False)
    kernel = kernel / jnp.sum(kernel)
    blurred = convolve(estimate, kernel)
    ratio_field = view_data / blurred
    correction = convolve(ratio_field, jnp.flip(kernel))
    updated = estimate * correction
    level_one = average_blocks(updated, True)
    level_two = average_blocks(level_one, True)
    level_three = average_blocks(level_two, True)
    level_four = average_blocks(level_three, True)
    level_five = average_blocks(level_four, False)
    return updated, level_one, level_two, level_three, level_four, level_five
```

```python
import functools
import math

import jax
import jax.numpy as jnp
import numpy as np
from jax import lax
from jax.experimental import pallas as pl
from jax.experimental.pallas import tpu as pltpu
from jax.sharding import PartitionSpec as P

MESH = pl.DeviceIdType.MESH
BF = jnp.bfloat16
F32 = jnp.float32
LANES = 128
EDGE = 16
DIRECTIONS = ((1, 0), (-1, 0), (0, 1), (0, -1), (1, 1), (-1, 1), (1, -1), (-1, -1))


def two_parts(matrix):
    matrix = np.asarray(matrix, np.float32)
    high = matrix.astype(BF)
    low = (matrix - high.astype(np.float32)).astype(BF)
    return high, low


def split(x):
    high = x.astype(BF)
    return high, (x - high.astype(F32)).astype(BF)


def dot(a, b):
    return jnp.dot(a, b, preferred_element_type=F32)


def tables(nx, ny, extent):
    radius = (extent - 1) // 2
    lx, ly = nx + 2 * EDGE, ny + 2 * EDGE
    nf = ly // 2 + 1
    freq_y = np.arange(nf)
    freq_x = np.arange(lx)

    def wave(k, n, length):
        return 2 * math.pi / length * np.mod(np.outer(k, n), length)

    pos = np.concatenate([EDGE + np.arange(ny), np.arange(EDGE), EDGE + ny + np.arange(EDGE)])
    fy = np.zeros((ny + LANES, 2 * LANES))
    angle = wave(pos, freq_y, ly)
    fy[: pos.size, :nf] = np.cos(angle)
    fy[: pos.size, LANES : LANES + nf] = -np.sin(angle)
    ky = np.zeros((LANES, 2 * LANES))
    angle = wave(np.arange(extent) - radius, freq_y, ly)
    ky[:extent, :nf] = np.cos(angle)
    ky[:extent, LANES : LANES + nf] = -np.sin(angle)
    iy = np.zeros((2 * LANES, ny))
    weight = np.full((nf, 1), 2.0)
    weight[0] = weight[-1] = 1.0
    angle = wave(freq_y, EDGE + np.arange(ny), ly)
    iy[:nf] = weight / ly * np.cos(angle)
    iy[LANES : LANES + nf] = -weight / ly * np.sin(angle)

    angle = wave(freq_x, np.arange(lx), lx)
    fx = np.block([[np.cos(angle), np.sin(angle)], [-np.sin(angle), np.cos(angle)]])
    angle = wave(EDGE + np.arange(nx), freq_x, lx)
    ix = np.block([[np.cos(angle), -np.sin(angle)], [np.sin(angle), np.cos(angle)]]) / lx
    kx = np.zeros((2 * lx, 2, extent + 1))
    angle = wave(freq_x, np.arange(extent) - radius, lx)
    kx[:lx, 0, :extent] = np.cos(angle)
    kx[:lx, 1, :extent] = np.sin(angle)
    kx[lx:, 0, :extent] = -np.sin(angle)
    kx[lx:, 1, :extent] = np.cos(angle)
    kx = kx.reshape(2 * lx, 2 * (extent + 1))

    fy_hi, fy_lo = two_parts(fy)
    ky_hi, ky_lo = two_parts(ky)
    iy_hi, iy_lo = two_parts(iy)
    fx_hi, fx_lo = two_parts(fx)
    ix_hi, ix_lo = two_parts(ix)
    kx_hi, kx_lo = two_parts(kx)

    py = np.zeros((ny, LANES))
    px = np.zeros((nx, nx))
    row, col = 0, 0
    places = []
    for level in range(1, 6):
        size = 2**level
        rows, cols = nx // size, ny // size
        places.append((row, rows, col, cols))
        for r in range(rows):
            px[row + r, r * size : (r + 1) * size] = 1.0 / size
        for c in range(cols):
            py[c * size : (c + 1) * size, col + c] = 1.0 / size
        row, col = row + rows, col + cols
    arrays = (
        fy_hi,
        fy_lo,
        np.concatenate([fx_hi, fx_lo], 0),
        ky_hi,
        ky_lo,
        np.concatenate([kx_hi, kx_hi, kx_lo], 1),
        np.concatenate([ix_hi, ix_lo], 0),
        iy_hi,
        iy_lo,
        py.astype(BF),
        px.astype(BF),
    )
    return arrays, tuple(places)


def kernel(
    sizes,
    places,
    index_ref, est_ref, view_ref, psf_hbm,
    fy_hi, fy_lo, fx2, ky_hi, ky_lo, kx3, ix2, iy_hi, iy_lo, py, px,
    out_ref, one_ref, two_ref, three_ref, four_ref, five_ref,
    psf, psf_pad, kd, k2, a_hi, a_lo, d_hi, d_lo, own, peer, mix, ratio,
    pack, xhalo, yhalo, share, share_in, tiles,
    psf_sem, hs, hr, es, er, ps, pr, gs, gr,
):
    gxn, gyn = sizes
    nz, nx, ny = est_ref.shape
    extent = psf_hbm.shape[1]
    lx = nx + 2 * EDGE
    gx, gy, gz = lax.axis_index("gx"), lax.axis_index("gy"), lax.axis_index("gz")
    partner = {"gx": gx, "gy": gy, "gz": 1 - gz}
    chips = gxn * gyn

    psf_copy = pltpu.make_async_copy(psf_hbm, psf, psf_sem)
    psf_copy.start()

    def chip_at(offset):
        x = lax.rem(gx + offset // gyn, gxn)
        y = lax.rem(gy + lax.rem(offset, gyn), gyn)
        return {"gx": x, "gy": y, "gz": gz}

    barrier = pltpu.get_barrier_semaphore()
    pl.semaphore_signal(barrier, inc=1, device_id=partner, device_id_type=MESH)

    @pl.loop(1, chips)
    def _(offset):
        pl.semaphore_signal(barrier, inc=1, device_id=chip_at(offset), device_id_type=MESH)

    def exists(dx, dy):
        ok = None
        for c, n, d in ((gx, gxn, dx), (gy, gyn, dy)):
            if d > 0:
                t = c < n - 1
            elif d < 0:
                t = c > 0
            else:
                continue
            ok = t if ok is None else jnp.logical_and(ok, t)
        return ok

    def halo_parts(phase, field, dx, dy):
        if dy == 0:
            rows = slice(nx - EDGE, nx) if dx > 0 else slice(0, EDGE)
            return field.at[:, rows, :], xhalo.at[phase, 0 if dx > 0 else 1]
        side = 0 if dy > 0 else 1
        if dx == 0:
            return pack.at[phase, side], yhalo.at[phase, side, pl.ds(EDGE, nx), :]
        rows = pl.ds(nx - EDGE, EDGE) if dx > 0 else pl.ds(0, EDGE)
        to = pl.ds(0, EDGE) if dx > 0 else pl.ds(EDGE + nx, EDGE)
        return pack.at[phase, side, rows, :], yhalo.at[phase, side, to, :]

    def halo_copy(phase, field, d):
        dx, dy = DIRECTIONS[d]
        source, target = halo_parts(phase, field, dx, dy)
        return pltpu.make_async_remote_copy(
            src_ref=source,
            dst_ref=target,
            send_sem=hs.at[phase, d],
            recv_sem=hr.at[phase, d],
            device_id={"gx": gx + dx, "gy": gy + dy, "gz": gz},
            device_id_type=MESH,
        )

    def do_pack(phase, field):
        lane = lax.broadcasted_iota(jnp.int32, (nx, LANES), 1) // EDGE
        last = jnp.zeros((nx, LANES), F32)
        first = jnp.zeros((nx, LANES), F32)
        for z in range(nz):
            plane = field[z]
            last = jnp.where(lane == z, pltpu.roll(plane, (EDGE * z + EDGE) % LANES, 1), last)
            first = jnp.where(lane == z, pltpu.roll(plane, EDGE * z, 1) if z else plane, first)
        pack[phase, 0] = last
        pack[phase, 1] = first

    def zero_missing(phase):
        for d, (dx, dy) in enumerate(DIRECTIONS):
            target = halo_parts(phase, est_ref, dx, dy)[1]

            @pl.when(jnp.logical_not(exists(-dx, -dy)))
            def _():
                target[...] = jnp.zeros(target.shape, F32)

    def send_halos(phase, field):
        for d, (dx, dy) in enumerate(DIRECTIONS):

            @pl.when(exists(dx, dy))
            def _():
                halo_copy(phase, field, d).start()

    def wait_halos(phase, field):
        for d, (dx, dy) in enumerate(DIRECTIONS):

            @pl.when(exists(-dx, -dy))
            def _():
                halo_copy(phase, field, d).wait_recv()

    def wait_sends(phase, field):
        for d, (dx, dy) in enumerate(DIRECTIONS):

            @pl.when(exists(dx, dy))
            def _():
                halo_copy(phase, field, d).wait_send()

    def plane_copy(phase, z):
        return pltpu.make_async_remote_copy(
            src_ref=own.at[phase, z],
            dst_ref=peer.at[phase, z],
            send_sem=es.at[phase, z],
            recv_sem=er.at[phase, z],
            device_id=partner,
            device_id_type=MESH,
        )

    def forward(phase, field):
        lane = lax.broadcasted_iota(jnp.int32, (lx, LANES), 1)
        for z in range(nz):
            body = jnp.concatenate([xhalo[phase, 0, z], field[z], xhalo[phase, 1, z]], axis=0)
            left, right = yhalo[phase, 0], yhalo[phase, 1]
            if z:
                left = pltpu.roll(left, LANES - EDGE * z, 1)
            if z != 1:
                right = pltpu.roll(right, (EDGE - EDGE * z) % LANES, 1)
            side = jnp.where(lane < EDGE, left, jnp.where(lane < 2 * EDGE, right, 0.0))
            full = jnp.concatenate([body, side], axis=1)
            a_hi[z], a_lo[z] = split(full)
        for z in range(nz):
            hi = a_hi[z]
            x1 = dot(hi, fy_hi[...]) + dot(a_lo[z], fy_hi[...]) + dot(hi, fy_lo[...])
            hi, lo = split(x1)
            d_hi[z, pl.ds(0, lx), :] = hi[:, :LANES]
            d_hi[z, pl.ds(lx, lx), :] = hi[:, LANES:]
            d_lo[z, pl.ds(0, lx), :] = lo[:, :LANES]
            d_lo[z, pl.ds(lx, lx), :] = lo[:, LANES:]
        for z in range(0, nz, 2):
            hi = jnp.concatenate([d_hi[z], d_hi[z + 1]], axis=1)
            lo = jnp.concatenate([d_lo[z], d_lo[z + 1]], axis=1)
            both = dot(fx2[...], hi)
            x2 = both[: 2 * lx] + both[2 * lx :] + dot(fx2[pl.ds(0, 2 * lx), :], lo)
            own[phase, z] = x2[:, :LANES]
            own[phase, z + 1] = x2[:, LANES:]
            plane_copy(phase, z).start()
            plane_copy(phase, z + 1).start()

    def mix_planes(source, phase, base, conj, add):
        @pl.loop(0, lx // 8)
        def _(s):
            re = pl.ds(pl.multiple_of(s * 8, 8), 8)
            im = pl.ds(pl.multiple_of(lx + s * 8, 8), 8)
            vr = [source[phase, j, re, :] for j in range(nz)]
            vi = [source[phase, j, im, :] for j in range(nz)]
            kr, ki = {}, {}
            for d in range(1 - nz, nz):
                kr[d] = k2[base + d, re, :]
                ki[d] = k2[base + d, im, :]
            for i in range(nz):
                yr = mix[i, re, :] if add else None
                yi = mix[i, im, :] if add else None
                for j in range(nz):
                    d = j - i if conj else i - j
                    rr, ii = kr[d] * vr[j], ki[d] * vi[j]
                    ri, ir = kr[d] * vi[j], ki[d] * vr[j]
                    tr, ti = (rr + ii, ri - ir) if conj else (rr - ii, ri + ir)
                    yr = tr if yr is None else yr + tr
                    yi = ti if yi is None else yi + ti
                mix[i, re, :] = yr
                mix[i, im, :] = yi

    def inverse(write):
        for z in range(0, nz, 2):
            y = jnp.concatenate([mix[z], mix[z + 1]], axis=1)
            hi, lo = split(y)
            both = dot(ix2[...], hi)
            g = both[: 2 * nx] + both[2 * nx :] + dot(ix2[pl.ds(0, 2 * nx), :], lo)
            for k in range(2):
                part = g[:, k * LANES : (k + 1) * LANES]
                rows = jnp.concatenate([part[:nx], part[nx:]], axis=1)
                hi, lo = split(rows)
                write(
                    z + k,
                    dot(hi, iy_hi[...]) + dot(lo, iy_hi[...]) + dot(hi, iy_lo[...]),
                )

    def convolve(phase, field, conj, write):
        forward(phase, field)
        sign = 1 - 2 * gz if conj else 2 * gz - 1
        middle = (extent - 1) // 2
        mix_planes(own, phase, middle, conj, False)
        for z in range(nz):
            plane_copy(phase, z).wait_recv()
        mix_planes(peer, phase, middle + sign * nz, conj, True)
        inverse(write)

    do_pack(0, est_ref)
    zero_missing(0)
    pl.semaphore_wait(barrier, chips)
    send_halos(0, est_ref)
    zero_missing(1)

    psf_copy.wait()
    chosen = psf[index_ref[0]]
    total = jnp.sum(chosen, axis=0)
    total = jnp.sum(jnp.sum(total, axis=1, keepdims=True), axis=0, keepdims=True)
    psf_pad[...] = jnp.zeros(psf_pad.shape, F32)
    psf_pad[pl.ds(0, extent), pl.ds(0, extent), pl.ds(0, extent)] = chosen * (1.0 / total)[None]
    wide = extent + 1

    @pl.loop(0, wide // 4)
    def _(q):
        block = psf_pad[pl.ds(q * 4, 4)].reshape(4 * wide, LANES)
        hi, lo = split(block)
        x1 = dot(hi, ky_hi[...]) + dot(lo, ky_hi[...]) + dot(hi, ky_lo[...])
        hi, lo = split(x1)
        hi = hi.reshape(4, wide, 2 * LANES)
        lo = lo.reshape(4, wide, 2 * LANES)
        for n, part in enumerate((hi, lo, hi)):
            kd[pl.ds(q * 4, 4), pl.ds(2 * n * wide, wide), :] = part[:, :, :LANES]
            kd[pl.ds(q * 4, 4), pl.ds(2 * n * wide + wide, wide), :] = part[:, :, LANES:]

    @pl.loop(0, wide // 4)
    def _(q):
        for h in range(2):
            n = q * 4 + 2 * h
            pair = jnp.concatenate([kd[n], kd[n + 1]], axis=1)
            spectrum = dot(kx3[...], pair)
            k2[n] = spectrum[:, :LANES]
            k2[n + 1] = spectrum[:, LANES:]

    wait_halos(0, est_ref)

    def write_ratio(z, blurred):
        ratio[z] = view_ref[z] / blurred

    convolve(0, est_ref, False, write_ratio)

    do_pack(1, ratio)
    send_halos(1, ratio)
    wait_halos(1, ratio)

    def write_update(z, correction):
        out_ref[z] = est_ref[z] * correction

    convolve(1, ratio, True, write_update)

    halves = [(out_ref[2 * i] + out_ref[2 * i + 1]) * 0.5 for i in range(nz // 2)]
    quarters = [(halves[2 * i] + halves[2 * i + 1]) * 0.5 for i in range(nz // 4)]
    eighth = (quarters[0] + quarters[1]) * 0.5

    def pooled(plane):
        hi, lo = split(plane)
        t = dot(hi, py[...]) + dot(lo, py[...])
        hi, lo = split(t)
        return dot(px[...], hi) + dot(px[...], lo)

    r4, c4 = places[3][0], places[3][2]
    last = pooled(eighth)
    share[0] = last[r4 : r4 + 8]
    share_copy = pltpu.make_async_remote_copy(
        src_ref=share.at[0], dst_ref=share_in, send_sem=ps, recv_sem=pr,
        device_id=partner, device_id_type=MESH,
    )
    share_copy.start()
    row, rows, col, cols = places[2]
    three_ref[0] = last[row : row + rows, col : col + cols]
    row, rows, col, cols = places[0]
    for i, plane in enumerate(halves):
        one_ref[i] = pooled(plane)[row : row + rows, col : col + cols]
    row, rows, col, cols = places[1]
    for i, plane in enumerate(quarters):
        two_ref[i] = pooled(plane)[row : row + rows, col : col + cols]
    share_copy.wait()
    both = (share[0] + share_in[...]) * 0.5
    four_ref[0] = both[: places[3][1], c4 : c4 + places[3][3]]
    row, rows, col, cols = places[4]
    row = row - r4
    r = lax.broadcasted_iota(jnp.int32, both.shape, 0)
    c = lax.broadcasted_iota(jnp.int32, both.shape, 1)
    inside = (r >= row) & (r < row + rows) & (c >= col) & (c < col + cols)
    mine = jnp.where(inside, both, 0.0)
    height = tiles.shape[1]
    if height > 8:
        mine = jnp.concatenate([mine, jnp.zeros((height - 8, LANES), F32)], axis=0)
    mine = pltpu.roll(mine, lax.rem(gy * cols + LANES - col, LANES), 1)
    mine = pltpu.roll(mine, lax.rem(gx * rows + height - row, height), 0)
    tiles[0] = mine

    def tile_copy(offset):
        return pltpu.make_async_remote_copy(
            src_ref=tiles.at[0], dst_ref=tiles.at[offset],
            send_sem=gs.at[offset], recv_sem=gr.at[offset],
            device_id=chip_at(offset), device_id_type=MESH,
        )

    @pl.loop(1, chips)
    def _(offset):
        tile_copy(offset).start()

    for phase, field in ((0, est_ref), (1, ratio)):
        wait_sends(phase, field)
        for z in range(nz):
            plane_copy(phase, z).wait_send()

    @pl.loop(1, chips)
    def _(offset):
        tile_copy(offset).wait()

    five = tiles[0]
    for offset in range(1, chips):
        five = five + tiles[offset]
    five_ref[0] = five[: five_ref.shape[1], : five_ref.shape[2]]


def local(sizes, estimate, view_data, psf_stack, view_index):
    gxn, gyn = sizes
    nz, nx, ny = estimate.shape
    views, extent = psf_stack.shape[:2]
    arrays, places = tables(nx, ny, extent)
    lx = nx + 2 * EDGE
    wide = extent + 1
    chips = gxn * gyn
    vmem = pl.BlockSpec(memory_space=pltpu.VMEM)

    def shape(*dims):
        return jax.ShapeDtypeStruct(dims, F32)

    rows5, cols5 = places[4][1] * gxn, places[4][3] * gyn
    dma = pltpu.SemaphoreType.DMA
    return pl.pallas_call(
        functools.partial(kernel, sizes, places),
        out_shape=(
            shape(nz, nx, ny),
            shape(nz // 2, nx // 2, ny // 2),
            shape(nz // 4, nx // 4, ny // 4),
            shape(nz // 8, nx // 8, ny // 8),
            shape(1, nx // 16, ny // 16),
            shape(1, rows5, cols5),
        ),
        in_specs=[pl.BlockSpec(memory_space=pltpu.SMEM), vmem, vmem, pl.BlockSpec(memory_space=pl.ANY)]
        + [vmem] * len(arrays),
        out_specs=(vmem,) * 6,
        scratch_shapes=[
            pltpu.VMEM(psf_stack.shape, F32),
            pltpu.VMEM((wide, wide, LANES), F32),
            pltpu.VMEM((wide, 6 * wide, LANES), BF),
            pltpu.VMEM((wide, 2 * lx, LANES), F32),
            pltpu.VMEM((nz, lx, 2 * LANES), BF),
            pltpu.VMEM((nz, lx, 2 * LANES), BF),
            pltpu.VMEM((nz, 2 * lx, LANES), BF),
            pltpu.VMEM((nz, 2 * lx, LANES), BF),
            pltpu.VMEM((2, nz, 2 * lx, LANES), F32),
            pltpu.VMEM((2, nz, 2 * lx, LANES), F32),
            pltpu.VMEM((nz, 2 * lx, LANES), F32),
            pltpu.VMEM((nz, nx, ny), F32),
            pltpu.VMEM((2, 2, nx, LANES), F32),
            pltpu.VMEM((2, 2, nz, EDGE, ny), F32),
            pltpu.VMEM((2, 2, lx, LANES), F32),
            pltpu.VMEM((1, 8, LANES), F32),
            pltpu.VMEM((8, LANES), F32),
            pltpu.VMEM((chips, max(8, rows5), LANES), F32),
            dma,
            dma((2, 8)),
            dma((2, 8)),
            dma((2, nz)),
            dma((2, nz)),
            dma,
            dma,
            dma((chips,)),
            dma((chips,)),
        ],
        compiler_params=pltpu.CompilerParams(
            collective_id=0, has_side_effects=True, vmem_limit_bytes=48 * 1024 * 1024
        ),
        name="deconvolve",
    )(view_index, estimate, view_data, psf_stack, *[jnp.asarray(a) for a in arrays])


def solution(mesh):
    return jax.shard_map(
        functools.partial(local, (mesh.shape["gx"], mesh.shape["gy"])),
        mesh=mesh,
        in_specs=(P("gz", "gx", "gy"), P("gz", "gx", "gy"), P(), P()),
        out_specs=(
            P("gz", "gx", "gy"),
            P("gz", "gx", "gy"),
            P("gz", "gx", "gy"),
            P("gz", "gx", "gy"),
            P(None, "gx", "gy"),
            P(),
        ),
        check_vma=False,
    )
```

```python
import functools
import math

import jax
import jax.numpy as jnp
import numpy as np
from jax import lax
from jax.experimental import pallas as pl
from jax.experimental.pallas import tpu as pltpu
from jax.sharding import PartitionSpec as P

MESH = pl.DeviceIdType.MESH
BF = jnp.bfloat16
F32 = jnp.float32
LANES = 128
EDGE = 16
TABLES = 11
DIRECTIONS = ((1, 0), (-1, 0), (0, 1), (0, -1), (1, 1), (-1, 1), (1, -1), (-1, -1))


def two_parts(matrix):
    matrix = np.asarray(matrix, np.float32)
    high = matrix.astype(BF)
    low = (matrix - high.astype(np.float32)).astype(BF)
    return high, low


def split(x):
    high = x.astype(BF)
    return high, (x - high.astype(F32)).astype(BF)


def dot(a, b):
    return jnp.dot(a, b, preferred_element_type=F32)


def tables(nx, ny, extent):
    radius = (extent - 1) // 2
    lx, ly = nx + 2 * EDGE, ny + 2 * EDGE
    nf = ly // 2 + 1
    freq_y = np.arange(nf)
    freq_x = np.arange(lx)

    def wave(k, n, length):
        return 2 * math.pi / length * np.mod(np.outer(k, n), length)

    pos = np.concatenate([EDGE + np.arange(ny), np.arange(EDGE), EDGE + ny + np.arange(EDGE)])
    fy = np.zeros((ny + LANES, 2 * LANES))
    angle = wave(pos, freq_y, ly)
    fy[: pos.size, :nf] = np.cos(angle)
    fy[: pos.size, LANES : LANES + nf] = -np.sin(angle)
    ky = np.zeros((LANES, 2 * LANES))
    angle = wave(np.arange(extent) - radius, freq_y, ly)
    ky[:extent, :nf] = np.cos(angle)
    ky[:extent, LANES : LANES + nf] = -np.sin(angle)
    iy = np.zeros((2 * LANES, ny))
    weight = np.full((nf, 1), 2.0)
    weight[0] = weight[-1] = 1.0
    angle = wave(freq_y, EDGE + np.arange(ny), ly)
    iy[:nf] = weight / ly * np.cos(angle)
    iy[LANES : LANES + nf] = -weight / ly * np.sin(angle)

    angle = wave(freq_x, np.arange(lx), lx)
    fx = np.block([[np.cos(angle), np.sin(angle)], [-np.sin(angle), np.cos(angle)]])
    angle = wave(EDGE + np.arange(nx), freq_x, lx)
    ix = np.block([[np.cos(angle), -np.sin(angle)], [np.sin(angle), np.cos(angle)]]) / lx
    kx = np.zeros((2 * lx, 2, extent + 1))
    angle = wave(freq_x, np.arange(extent) - radius, lx)
    kx[:lx, 0, :extent] = np.cos(angle)
    kx[:lx, 1, :extent] = np.sin(angle)
    kx[lx:, 0, :extent] = -np.sin(angle)
    kx[lx:, 1, :extent] = np.cos(angle)
    kx = kx.reshape(2 * lx, 2 * (extent + 1))

    fy_hi, fy_lo = two_parts(fy)
    ky_hi, ky_lo = two_parts(ky)
    iy_hi, iy_lo = two_parts(iy)
    fx_hi, fx_lo = two_parts(fx)
    ix_hi, ix_lo = two_parts(ix)
    kx_hi, kx_lo = two_parts(kx)

    py = np.zeros((ny, LANES))
    px = np.zeros((nx, nx))
    row, col = 0, 0
    places = []
    for level in range(1, 6):
        size = 2**level
        rows, cols = nx // size, ny // size
        places.append((row, rows, col, cols))
        for r in range(rows):
            px[row + r, r * size : (r + 1) * size] = 1.0 / size
        for c in range(cols):
            py[c * size : (c + 1) * size, col + c] = 1.0 / size
        row, col = row + rows, col + cols
    arrays = (
        fy_hi,
        fy_lo,
        np.concatenate([fx_hi, fx_lo], 0),
        ky_hi,
        ky_lo,
        np.concatenate([kx_hi, kx_hi, kx_lo], 1),
        np.concatenate([ix_hi, ix_lo], 0),
        iy_hi,
        iy_lo,
        py.astype(BF),
        px.astype(BF),
    )
    return arrays, tuple(places)


def kernel(
    sizes,
    places,
    index_ref, est_hbm, view_hbm, psf_hbm, *rest,
):
    count = TABLES
    tables_hbm, rest = rest[:count], rest[count:]
    body(
        sizes, places, index_ref, (est_hbm, psf_hbm, *tables_hbm, view_hbm), *rest
    )


def body(
    sizes,
    places,
    index_ref, operands,
    out_ref, one_ref, two_ref, three_ref, four_ref, five_ref,
    psf_pad, kd, k2, own, peer, mix, ratio,
    pack, xhalo, yhalo, share, share_in, tiles,
    in_sem, xs, xr, hs, hr, es, er, ps, pr, gs, gr,
    est_ref, psf, fy_hi, fy_lo, fx2, ky_hi, ky_lo, kx3, ix2, iy_hi, iy_lo, py, px, view_ref,
):
    gxn, gyn = sizes
    nz, nx, ny = est_ref.shape
    extent = psf.shape[1]
    pairs = nz // 2
    lx = nx + 2 * EDGE
    gx, gy, gz = lax.axis_index("gx"), lax.axis_index("gy"), lax.axis_index("gz")
    partner = {"gx": gx, "gy": gy, "gz": 1 - gz}
    chips = gxn * gyn

    resident = (
        est_ref, psf, fy_hi, fy_lo, fx2, ky_hi, ky_lo, kx3, ix2, iy_hi, iy_lo, py, px, view_ref
    )
    loads = [
        pltpu.make_async_copy(a, b, in_sem.at[i])
        for i, (a, b) in enumerate(zip(operands, resident))
    ]
    loads[0].start()

    def chip_at(offset):
        x = lax.rem(gx + offset // gyn, gxn)
        y = lax.rem(gy + lax.rem(offset, gyn), gyn)
        return {"gx": x, "gy": y, "gz": gz}

    barrier = pltpu.get_barrier_semaphore()
    pl.semaphore_signal(barrier, inc=1, device_id=partner, device_id_type=MESH)

    @pl.loop(1, chips)
    def _(offset):
        pl.semaphore_signal(barrier, inc=1, device_id=chip_at(offset), device_id_type=MESH)

    for load in loads[1:]:
        load.start()

    def exists(dx, dy):
        ok = None
        for c, n, d in ((gx, gxn, dx), (gy, gyn, dy)):
            if d > 0:
                t = c < n - 1
            elif d < 0:
                t = c > 0
            else:
                continue
            ok = t if ok is None else jnp.logical_and(ok, t)
        return ok

    def halo_parts(phase, field, dx, dy):
        if dy == 0:
            rows = slice(nx - EDGE, nx) if dx > 0 else slice(0, EDGE)
            return field.at[:, rows, :], xhalo.at[phase, 0 if dx > 0 else 1]
        side = 0 if dy > 0 else 1
        if dx == 0:
            return pack.at[phase, side], yhalo.at[phase, side, pl.ds(EDGE, nx), :]
        rows = pl.ds(nx - EDGE, EDGE) if dx > 0 else pl.ds(0, EDGE)
        to = pl.ds(0, EDGE) if dx > 0 else pl.ds(EDGE + nx, EDGE)
        return pack.at[phase, side, rows, :], yhalo.at[phase, side, to, :]

    def halo_copy(phase, field, d):
        dx, dy = DIRECTIONS[d]
        source, target = halo_parts(phase, field, dx, dy)
        return pltpu.make_async_remote_copy(
            src_ref=source,
            dst_ref=target,
            send_sem=hs.at[phase, d],
            recv_sem=hr.at[phase, d],
            device_id={"gx": gx + dx, "gy": gy + dy, "gz": gz},
            device_id_type=MESH,
        )

    def pair_copy(phase, field, d, q):
        source, target = halo_parts(phase, field, *DIRECTIONS[d])
        planes = pl.ds(2 * q, 2)
        rows = pl.ds(nx - EDGE, EDGE) if d == 0 else pl.ds(0, EDGE)
        return pltpu.make_async_remote_copy(
            src_ref=field.at[planes, rows, :],
            dst_ref=xhalo.at[phase, d, planes],
            send_sem=xs.at[phase, d, q],
            recv_sem=xr.at[phase, d, q],
            device_id={"gx": gx + DIRECTIONS[d][0], "gy": gy, "gz": gz},
            device_id_type=MESH,
        )

    def for_existing(towards, directions, act):
        for d in directions:
            dx, dy = DIRECTIONS[d]

            @pl.when(exists(dx, dy) if towards else exists(-dx, -dy))
            def _():
                act(d)

    def send_pair(phase, field, q):
        for_existing(True, (0, 1), lambda d: pair_copy(phase, field, d, q).start())

    def wait_pair(phase, field, q):
        for_existing(False, (0, 1), lambda d: pair_copy(phase, field, d, q).wait_recv())

    def do_pack(phase, field):
        lane = lax.broadcasted_iota(jnp.int32, (nx, LANES), 1) // EDGE
        last = jnp.zeros((nx, LANES), F32)
        first = jnp.zeros((nx, LANES), F32)
        for z in range(nz):
            plane = field[z]
            last = jnp.where(lane == z, pltpu.roll(plane, (EDGE * z + EDGE) % LANES, 1), last)
            first = jnp.where(lane == z, pltpu.roll(plane, EDGE * z, 1) if z else plane, first)
        pack[phase, 0] = last
        pack[phase, 1] = first

    def zero_missing(phase):
        for d, (dx, dy) in enumerate(DIRECTIONS):
            target = halo_parts(phase, est_ref, dx, dy)[1]

            @pl.when(jnp.logical_not(exists(-dx, -dy)))
            def _():
                target[...] = jnp.zeros(target.shape, F32)

    others = range(2, 8)

    def send_others(phase, field):
        for_existing(True, others, lambda d: halo_copy(phase, field, d).start())

    def wait_others(phase, field):
        for_existing(False, others, lambda d: halo_copy(phase, field, d).wait_recv())

    def wait_sends(phase, field):
        for_existing(True, others, lambda d: halo_copy(phase, field, d).wait_send())
        for q in range(pairs):
            for_existing(True, (0, 1), lambda d: pair_copy(phase, field, d, q).wait_send())
            swap_copy(phase, q).wait_send()

    def swap_copy(phase, q):
        planes = pl.ds(2 * q, 2)
        return pltpu.make_async_remote_copy(
            src_ref=own.at[phase, planes],
            dst_ref=peer.at[phase, planes],
            send_sem=es.at[phase, q],
            recv_sem=er.at[phase, q],
            device_id=partner,
            device_id_type=MESH,
        )

    def forward(phase, field, q):
        lane = lax.broadcasted_iota(jnp.int32, (lx, LANES), 1)
        full = []
        for z in (2 * q, 2 * q + 1):
            rows = jnp.concatenate([xhalo[phase, 0, z], field[z], xhalo[phase, 1, z]], axis=0)
            left, right = yhalo[phase, 0], yhalo[phase, 1]
            if z:
                left = pltpu.roll(left, LANES - EDGE * z, 1)
            if z != 1:
                right = pltpu.roll(right, (EDGE - EDGE * z) % LANES, 1)
            side = jnp.where(lane < EDGE, left, jnp.where(lane < 2 * EDGE, right, 0.0))
            full.append(jnp.concatenate([rows, side], axis=1))
        hi, lo = split(jnp.concatenate(full, axis=0))
        x1 = dot(hi, fy_hi[...]) + dot(lo, fy_hi[...]) + dot(hi, fy_lo[...])
        stacked = [
            jnp.concatenate(
                [x1[k * lx : (k + 1) * lx, :LANES], x1[k * lx : (k + 1) * lx, LANES:]], axis=0
            )
            for k in range(2)
        ]
        hi, lo = split(jnp.concatenate(stacked, axis=1))
        both = dot(fx2[...], hi)
        x2 = both[: 2 * lx] + both[2 * lx :] + dot(fx2[pl.ds(0, 2 * lx), :], lo)
        own[phase, 2 * q] = x2[:, :LANES]
        own[phase, 2 * q + 1] = x2[:, LANES:]
        swap_copy(phase, q).start()

    def mix_planes(source, phase, base, conj, add, chosen):
        @pl.loop(0, lx // 8)
        def _(s):
            re = pl.ds(pl.multiple_of(s * 8, 8), 8)
            im = pl.ds(pl.multiple_of(lx + s * 8, 8), 8)
            vr = [source[phase, j, re, :] for j in range(nz)]
            vi = [source[phase, j, im, :] for j in range(nz)]
            kr, ki = {}, {}
            reach = [(j - i if conj else i - j) for i in chosen for j in range(nz)]
            for d in sorted(set(reach)):
                kr[d] = k2[base + d, re, :]
                ki[d] = k2[base + d, im, :]
            for i in chosen:
                yr = mix[i, re, :] if add else None
                yi = mix[i, im, :] if add else None
                for j in range(nz):
                    d = j - i if conj else i - j
                    rr, ii = kr[d] * vr[j], ki[d] * vi[j]
                    ri, ir = kr[d] * vi[j], ki[d] * vr[j]
                    tr, ti = (rr + ii, ri - ir) if conj else (rr - ii, ri + ir)
                    yr = tr if yr is None else yr + tr
                    yi = ti if yi is None else yi + ti
                mix[i, re, :] = yr
                mix[i, im, :] = yi

    def inverse(planes, write, after):
        for z in planes:
            y = jnp.concatenate([mix[z], mix[z + 1]], axis=1)
            hi, lo = split(y)
            both = dot(ix2[...], hi)
            g = both[: 2 * nx] + both[2 * nx :] + dot(ix2[pl.ds(0, 2 * nx), :], lo)
            for k in range(2):
                part = g[:, k * LANES : (k + 1) * LANES]
                rows = jnp.concatenate([part[:nx], part[nx:]], axis=1)
                hi, lo = split(rows)
                write(
                    z + k,
                    dot(hi, iy_hi[...]) + dot(lo, iy_hi[...]) + dot(hi, iy_lo[...]),
                )
            after(z // 2)

    def convolve(phase, field, conj, groups, write, after):
        wait_others(phase, field)
        for q in range(pairs):
            wait_pair(phase, field, q)
            forward(phase, field, q)
        sign = 1 - 2 * gz if conj else 2 * gz - 1
        middle = (extent - 1) // 2
        mix_planes(own, phase, middle, conj, False, range(nz))
        for q in range(pairs):
            swap_copy(phase, q).wait_recv()
        size = nz // groups
        for n in range(groups):
            planes = range(n * size, (n + 1) * size)
            mix_planes(peer, phase, middle + sign * nz, conj, True, planes)
            inverse(planes[::2], write, after)

    zero_missing(0)
    loads[0].wait()
    do_pack(0, est_ref)
    pl.semaphore_wait(barrier, chips)
    for q in range(pairs):
        send_pair(0, est_ref, q)
    send_others(0, est_ref)
    zero_missing(1)

    for load in loads[1:]:
        load.wait()
    chosen = psf[index_ref[0]]
    total = jnp.sum(chosen, axis=0)
    total = jnp.sum(jnp.sum(total, axis=1, keepdims=True), axis=0, keepdims=True)
    psf_pad[...] = jnp.zeros(psf_pad.shape, F32)
    psf_pad[pl.ds(0, extent), pl.ds(0, extent), pl.ds(0, extent)] = chosen * (1.0 / total)[None]
    wide = extent + 1

    @pl.loop(0, wide // 4)
    def _(q):
        block = psf_pad[pl.ds(q * 4, 4)].reshape(4 * wide, LANES)
        hi, lo = split(block)
        x1 = dot(hi, ky_hi[...]) + dot(lo, ky_hi[...]) + dot(hi, ky_lo[...])
        hi, lo = split(x1)
        hi = hi.reshape(4, wide, 2 * LANES)
        lo = lo.reshape(4, wide, 2 * LANES)
        for n, part in enumerate((hi, lo, hi)):
            kd[pl.ds(q * 4, 4), pl.ds(2 * n * wide, wide), :] = part[:, :, :LANES]
            kd[pl.ds(q * 4, 4), pl.ds(2 * n * wide + wide, wide), :] = part[:, :, LANES:]

    @pl.loop(0, wide // 4)
    def _(q):
        for h in range(2):
            n = q * 4 + 2 * h
            pair = jnp.concatenate([kd[n], kd[n + 1]], axis=1)
            spectrum = dot(kx3[...], pair)
            k2[n] = spectrum[:, :LANES]
            k2[n + 1] = spectrum[:, LANES:]

    def write_ratio(z, blurred):
        ratio[z] = view_ref[z] / blurred

    convolve(0, est_ref, False, 2, write_ratio, lambda q: send_pair(1, ratio, q))

    do_pack(1, ratio)
    send_others(1, ratio)

    def write_update(z, correction):
        out_ref[z] = est_ref[z] * correction

    convolve(1, ratio, True, 1, write_update, lambda q: None)

    halves = [(out_ref[2 * i] + out_ref[2 * i + 1]) * 0.5 for i in range(nz // 2)]
    quarters = [(halves[2 * i] + halves[2 * i + 1]) * 0.5 for i in range(nz // 4)]
    eighth = (quarters[0] + quarters[1]) * 0.5

    def pooled(plane):
        hi, lo = split(plane)
        t = dot(hi, py[...]) + dot(lo, py[...])
        hi, lo = split(t)
        return dot(px[...], hi) + dot(px[...], lo)

    r4, c4 = places[3][0], places[3][2]
    last = pooled(eighth)
    share[0] = last[r4 : r4 + 8]
    share_copy = pltpu.make_async_remote_copy(
        src_ref=share.at[0], dst_ref=share_in, send_sem=ps, recv_sem=pr,
        device_id=partner, device_id_type=MESH,
    )
    share_copy.start()
    row, rows, col, cols = places[2]
    three_ref[0] = last[row : row + rows, col : col + cols]
    row, rows, col, cols = places[1]
    for i, plane in enumerate(quarters):
        two_ref[i] = pooled(plane)[row : row + rows, col : col + cols]
    share_copy.wait()
    both = (share[0] + share_in[...]) * 0.5
    four_ref[0] = both[: places[3][1], c4 : c4 + places[3][3]]
    row, rows, col, cols = places[4]
    row = row - r4
    r = lax.broadcasted_iota(jnp.int32, both.shape, 0)
    c = lax.broadcasted_iota(jnp.int32, both.shape, 1)
    inside = (r >= row) & (r < row + rows) & (c >= col) & (c < col + cols)
    mine = jnp.where(inside, both, 0.0)
    height = tiles.shape[1]
    if height > 8:
        mine = jnp.concatenate([mine, jnp.zeros((height - 8, LANES), F32)], axis=0)
    mine = pltpu.roll(mine, lax.rem(gy * cols + LANES - col, LANES), 1)
    mine = pltpu.roll(mine, lax.rem(gx * rows + height - row, height), 0)
    tiles[0] = mine

    def tile_copy(offset):
        return pltpu.make_async_remote_copy(
            src_ref=tiles.at[0], dst_ref=tiles.at[offset],
            send_sem=gs.at[offset], recv_sem=gr.at[offset],
            device_id=chip_at(offset), device_id_type=MESH,
        )

    @pl.loop(1, chips)
    def _(offset):
        tile_copy(offset).start()

    row, rows, col, cols = places[0]
    for i, plane in enumerate(halves):
        one_ref[i] = pooled(plane)[row : row + rows, col : col + cols]
    for phase, field in ((0, est_ref), (1, ratio)):
        wait_sends(phase, field)

    @pl.loop(1, chips)
    def _(offset):
        tile_copy(offset).wait()

    five = tiles[0]
    for offset in range(1, chips):
        five = five + tiles[offset]
    five_ref[0] = five[: five_ref.shape[1], : five_ref.shape[2]]


def write_out(*refs):
    sems = refs[12]
    copies = [pltpu.make_async_copy(refs[i], refs[6 + i], sems.at[i]) for i in range(6)]
    for copy in copies:
        copy.start()
    for copy in copies:
        copy.wait()


def local(sizes, estimate, view_data, psf_stack, view_index):
    gxn, gyn = sizes
    nz, nx, ny = estimate.shape
    views, extent = psf_stack.shape[:2]
    arrays, places = tables(nx, ny, extent)
    lx = nx + 2 * EDGE
    wide = extent + 1
    chips = gxn * gyn
    vmem = pl.BlockSpec(memory_space=pltpu.VMEM)
    hbm = pl.BlockSpec(memory_space=pltpu.HBM)

    def shape(*dims):
        return jax.ShapeDtypeStruct(dims, F32)

    rows5, cols5 = places[4][1] * gxn, places[4][3] * gyn
    dma = pltpu.SemaphoreType.DMA
    shapes = (
        shape(nz, nx, ny),
        shape(nz // 2, nx // 2, ny // 2),
        shape(nz // 4, nx // 4, ny // 4),
        shape(nz // 8, nx // 8, ny // 8),
        shape(1, nx // 16, ny // 16),
        shape(1, rows5, cols5),
    )
    results = pl.pallas_call(
        functools.partial(kernel, sizes, places),
        out_shape=shapes,
        in_specs=[pl.BlockSpec(memory_space=pltpu.SMEM)] + [hbm] * (len(arrays) + 3),
        out_specs=(vmem,) * 6,
        scratch_shapes=[
            pltpu.VMEM((wide, wide, LANES), F32),
            pltpu.VMEM((wide, 6 * wide, LANES), BF),
            pltpu.VMEM((wide, 2 * lx, LANES), F32),
            pltpu.VMEM((2, nz, 2 * lx, LANES), F32),
            pltpu.VMEM((2, nz, 2 * lx, LANES), F32),
            pltpu.VMEM((nz, 2 * lx, LANES), F32),
            pltpu.VMEM((nz, nx, ny), F32),
            pltpu.VMEM((2, 2, nx, LANES), F32),
            pltpu.VMEM((2, 2, nz, EDGE, ny), F32),
            pltpu.VMEM((2, 2, lx, LANES), F32),
            pltpu.VMEM((1, 8, LANES), F32),
            pltpu.VMEM((8, LANES), F32),
            pltpu.VMEM((chips, max(8, rows5), LANES), F32),
            dma((len(arrays) + 3,)),
            dma((2, 2, nz // 2)),
            dma((2, 2, nz // 2)),
            dma((2, 8)),
            dma((2, 8)),
            dma((2, nz // 2)),
            dma((2, nz // 2)),
            dma,
            dma,
            dma((chips,)),
            dma((chips,)),
            *[pltpu.VMEM(a.shape, a.dtype) for a in (estimate, psf_stack, *arrays, view_data)],
        ],
        compiler_params=pltpu.CompilerParams(
            collective_id=0, has_side_effects=True, vmem_limit_bytes=67043328 - 450000
        ),
        name="deconvolve",
    )(view_index, estimate, view_data, psf_stack, *[jnp.asarray(a) for a in arrays])
    return pl.pallas_call(
        write_out,
        out_shape=shapes,
        in_specs=[vmem] * 6,
        out_specs=(hbm,) * 6,
        scratch_shapes=[dma((6,))],
        name="write_out",
    )(*results)


def solution(mesh):
    return jax.shard_map(
        functools.partial(local, (mesh.shape["gx"], mesh.shape["gy"])),
        mesh=mesh,
        in_specs=(P("gz", "gx", "gy"), P("gz", "gx", "gy"), P(), P()),
        out_specs=(
            P("gz", "gx", "gy"),
            P("gz", "gx", "gy"),
            P("gz", "gx", "gy"),
            P("gz", "gx", "gy"),
            P(None, "gx", "gy"),
            P(),
        ),
        check_vma=False,
    )
```

```python
import functools
import math

import jax
import jax.numpy as jnp
import numpy as np
from jax import lax
from jax.experimental import pallas as pl
from jax.experimental.pallas import tpu as pltpu
from jax.sharding import PartitionSpec as P

MESH = pl.DeviceIdType.MESH
BF = jnp.bfloat16
F32 = jnp.float32
LANES = 128
EDGE = 16
TABLES = 11
DIRECTIONS = ((1, 0), (-1, 0), (0, 1), (0, -1), (1, 1), (-1, 1), (1, -1), (-1, -1))


def two_parts(matrix):
    matrix = np.asarray(matrix, np.float32)
    high = matrix.astype(BF)
    low = (matrix - high.astype(np.float32)).astype(BF)
    return high, low


def split(x):
    high = x.astype(BF)
    return high, (x - high.astype(F32)).astype(BF)


def dot(a, b):
    return jnp.dot(a, b, preferred_element_type=F32)


def tables(nx, ny, extent):
    radius = (extent - 1) // 2
    lx, ly = nx + 2 * EDGE, ny + 2 * EDGE
    nf = ly // 2 + 1
    freq_y = np.arange(nf)
    freq_x = np.arange(lx)

    def wave(k, n, length):
        return 2 * math.pi / length * np.mod(np.outer(k, n), length)

    pos = np.concatenate([EDGE + np.arange(ny), np.arange(EDGE), EDGE + ny + np.arange(EDGE)])
    fy = np.zeros((ny + LANES, 2 * LANES))
    angle = wave(pos, freq_y, ly)
    fy[: pos.size, :nf] = np.cos(angle)
    fy[: pos.size, LANES : LANES + nf] = -np.sin(angle)
    ky = np.zeros((LANES, 2 * LANES))
    angle = wave(np.arange(extent) - radius, freq_y, ly)
    ky[:extent, :nf] = np.cos(angle)
    ky[:extent, LANES : LANES + nf] = -np.sin(angle)
    iy = np.zeros((2 * LANES, ny))
    weight = np.full((nf, 1), 2.0)
    weight[0] = weight[-1] = 1.0
    angle = wave(freq_y, EDGE + np.arange(ny), ly)
    iy[:nf] = weight / ly * np.cos(angle)
    iy[LANES : LANES + nf] = -weight / ly * np.sin(angle)

    angle = wave(freq_x, np.arange(lx), lx)
    fx = np.block([[np.cos(angle), np.sin(angle)], [-np.sin(angle), np.cos(angle)]])
    angle = wave(EDGE + np.arange(nx), freq_x, lx)
    ix = np.block([[np.cos(angle), -np.sin(angle)], [np.sin(angle), np.cos(angle)]]) / lx
    kx = np.zeros((2 * lx, 2, extent + 1))
    angle = wave(freq_x, np.arange(extent) - radius, lx)
    kx[:lx, 0, :extent] = np.cos(angle)
    kx[:lx, 1, :extent] = np.sin(angle)
    kx[lx:, 0, :extent] = -np.sin(angle)
    kx[lx:, 1, :extent] = np.cos(angle)
    kx = kx.reshape(2 * lx, 2 * (extent + 1))

    fy_hi, fy_lo = two_parts(fy)
    ky_hi, ky_lo = two_parts(ky)
    iy_hi, iy_lo = two_parts(iy)
    fx_hi, fx_lo = two_parts(fx)
    ix_hi, ix_lo = two_parts(ix)
    kx_hi, kx_lo = two_parts(kx)

    py = np.zeros((ny, LANES))
    px = np.zeros((nx, nx))
    row, col = 0, 0
    places = []
    for level in range(1, 6):
        size = 2**level
        rows, cols = nx // size, ny // size
        places.append((row, rows, col, cols))
        for r in range(rows):
            px[row + r, r * size : (r + 1) * size] = 1.0 / size
        for c in range(cols):
            py[c * size : (c + 1) * size, col + c] = 1.0 / size
        row, col = row + rows, col + cols
    arrays = (
        fy_hi,
        fy_lo,
        np.concatenate([fx_hi, fx_lo], 0),
        ky_hi,
        ky_lo,
        np.concatenate([kx_hi, kx_hi, kx_lo], 1),
        np.concatenate([ix_hi, ix_lo], 0),
        iy_hi,
        iy_lo,
        py.astype(BF),
        px.astype(BF),
    )
    return arrays, tuple(places)


def kernel(
    sizes,
    places,
    index_ref, est_hbm, view_hbm, psf_hbm, *rest,
):
    count = TABLES
    tables_hbm, rest = rest[:count], rest[count:]
    body(
        sizes, places, index_ref, (est_hbm, psf_hbm, *tables_hbm, view_hbm), *rest
    )


def body(
    sizes,
    places,
    index_ref, operands,
    out_ref, one_ref, two_ref, three_ref, four_ref, five_ref,
    psf_pad, kd, k2, own, peer, mix, ratio,
    pack, xhalo, yhalo, share, share_in, tiles,
    in_sem, xs, xr, hs, hr, es, er, ps, pr, gs, gr,
    est_ref, psf, fy_hi, fy_lo, fx2, ky_hi, ky_lo, kx3, ix2, iy_hi, iy_lo, py, px, view_ref,
):
    gxn, gyn = sizes
    nz, nx, ny = est_ref.shape
    extent = psf.shape[1]
    pairs = nz // 2
    lx = nx + 2 * EDGE
    gx, gy, gz = lax.axis_index("gx"), lax.axis_index("gy"), lax.axis_index("gz")
    partner = {"gx": gx, "gy": gy, "gz": 1 - gz}
    chips = gxn * gyn

    resident = (
        est_ref, psf, fy_hi, fy_lo, fx2, ky_hi, ky_lo, kx3, ix2, iy_hi, iy_lo, py, px, view_ref
    )
    loads = [
        pltpu.make_async_copy(a, b, in_sem.at[i])
        for i, (a, b) in enumerate(zip(operands, resident))
    ]
    loads[0].start()

    def chip_at(offset):
        x = lax.rem(gx + offset // gyn, gxn)
        y = lax.rem(gy + lax.rem(offset, gyn), gyn)
        return {"gx": x, "gy": y, "gz": gz}

    barrier = pltpu.get_barrier_semaphore()
    pl.semaphore_signal(barrier, inc=1, device_id=partner, device_id_type=MESH)

    @pl.loop(1, chips)
    def _(offset):
        pl.semaphore_signal(barrier, inc=1, device_id=chip_at(offset), device_id_type=MESH)

    for load in loads[1:]:
        load.start()

    def exists(dx, dy):
        ok = None
        for c, n, d in ((gx, gxn, dx), (gy, gyn, dy)):
            if d > 0:
                t = c < n - 1
            elif d < 0:
                t = c > 0
            else:
                continue
            ok = t if ok is None else jnp.logical_and(ok, t)
        return ok

    def halo_parts(phase, field, dx, dy):
        if dy == 0:
            rows = slice(nx - EDGE, nx) if dx > 0 else slice(0, EDGE)
            return field.at[:, rows, :], xhalo.at[phase, 0 if dx > 0 else 1]
        side = 0 if dy > 0 else 1
        if dx == 0:
            return pack.at[phase, side], yhalo.at[phase, side, pl.ds(EDGE, nx), :]
        rows = pl.ds(nx - EDGE, EDGE) if dx > 0 else pl.ds(0, EDGE)
        to = pl.ds(0, EDGE) if dx > 0 else pl.ds(EDGE + nx, EDGE)
        return pack.at[phase, side, rows, :], yhalo.at[phase, side, to, :]

    def halo_copy(phase, field, d):
        dx, dy = DIRECTIONS[d]
        source, target = halo_parts(phase, field, dx, dy)
        return pltpu.make_async_remote_copy(
            src_ref=source,
            dst_ref=target,
            send_sem=hs.at[phase, d],
            recv_sem=hr.at[phase, d],
            device_id={"gx": gx + dx, "gy": gy + dy, "gz": gz},
            device_id_type=MESH,
        )

    def pair_copy(phase, field, d, q):
        source, target = halo_parts(phase, field, *DIRECTIONS[d])
        planes = pl.ds(2 * q, 2)
        rows = pl.ds(nx - EDGE, EDGE) if d == 0 else pl.ds(0, EDGE)
        return pltpu.make_async_remote_copy(
            src_ref=field.at[planes, rows, :],
            dst_ref=xhalo.at[phase, d, planes],
            send_sem=xs.at[phase, d, q],
            recv_sem=xr.at[phase, d, q],
            device_id={"gx": gx + DIRECTIONS[d][0], "gy": gy, "gz": gz},
            device_id_type=MESH,
        )

    def for_existing(towards, directions, act):
        for d in directions:
            dx, dy = DIRECTIONS[d]

            @pl.when(exists(dx, dy) if towards else exists(-dx, -dy))
            def _():
                act(d)

    def send_pair(phase, field, q):
        for_existing(True, (0, 1), lambda d: pair_copy(phase, field, d, q).start())

    def wait_pair(phase, field, q):
        for_existing(False, (0, 1), lambda d: pair_copy(phase, field, d, q).wait_recv())

    def do_pack(phase, field):
        lane = lax.broadcasted_iota(jnp.int32, (nx, LANES), 1) // EDGE
        last = jnp.zeros((nx, LANES), F32)
        first = jnp.zeros((nx, LANES), F32)
        for z in range(nz):
            plane = field[z]
            last = jnp.where(lane == z, pltpu.roll(plane, (EDGE * z + EDGE) % LANES, 1), last)
            first = jnp.where(lane == z, pltpu.roll(plane, EDGE * z, 1) if z else plane, first)
        pack[phase, 0] = last
        pack[phase, 1] = first

    def zero_missing(phase):
        for d, (dx, dy) in enumerate(DIRECTIONS):
            target = halo_parts(phase, est_ref, dx, dy)[1]

            @pl.when(jnp.logical_not(exists(-dx, -dy)))
            def _():
                target[...] = jnp.zeros(target.shape, F32)

    others = range(2, 8)

    def send_others(phase, field):
        for_existing(True, others, lambda d: halo_copy(phase, field, d).start())

    def wait_others(phase, field):
        for_existing(False, others, lambda d: halo_copy(phase, field, d).wait_recv())

    def wait_sends(phase, field):
        for_existing(True, others, lambda d: halo_copy(phase, field, d).wait_send())
        for q in range(pairs):
            for_existing(True, (0, 1), lambda d: pair_copy(phase, field, d, q).wait_send())
            swap_copy(phase, q).wait_send()

    def swap_copy(phase, q):
        planes = pl.ds(2 * q, 2)
        return pltpu.make_async_remote_copy(
            src_ref=own.at[phase, planes],
            dst_ref=peer.at[phase, planes],
            send_sem=es.at[phase, q],
            recv_sem=er.at[phase, q],
            device_id=partner,
            device_id_type=MESH,
        )

    def forward(phase, field, q):
        lane = lax.broadcasted_iota(jnp.int32, (lx, LANES), 1)
        full = []
        for z in (2 * q, 2 * q + 1):
            rows = jnp.concatenate([xhalo[phase, 0, z], field[z], xhalo[phase, 1, z]], axis=0)
            left, right = yhalo[phase, 0], yhalo[phase, 1]
            if z:
                left = pltpu.roll(left, LANES - EDGE * z, 1)
            if z != 1:
                right = pltpu.roll(right, (EDGE - EDGE * z) % LANES, 1)
            side = jnp.where(lane < EDGE, left, jnp.where(lane < 2 * EDGE, right, 0.0))
            full.append(jnp.concatenate([rows, side], axis=1))
        hi, lo = split(jnp.concatenate(full, axis=0))
        x1 = dot(hi, fy_hi[...]) + dot(lo, fy_hi[...]) + dot(hi, fy_lo[...])
        stacked = [
            jnp.concatenate(
                [x1[k * lx : (k + 1) * lx, :LANES], x1[k * lx : (k + 1) * lx, LANES:]], axis=0
            )
            for k in range(2)
        ]
        hi, lo = split(jnp.concatenate(stacked, axis=1))
        both = dot(fx2[...], hi)
        x2 = both[: 2 * lx] + both[2 * lx :] + dot(fx2[pl.ds(0, 2 * lx), :], lo)
        own[phase, 2 * q] = x2[:, :LANES]
        own[phase, 2 * q + 1] = x2[:, LANES:]
        swap_copy(phase, q).start()

    def mix_planes(source, phase, base, conj, add, chosen):
        @pl.loop(0, lx // 8)
        def _(s):
            re = pl.ds(pl.multiple_of(s * 8, 8), 8)
            im = pl.ds(pl.multiple_of(lx + s * 8, 8), 8)
            vr = [source[phase, j, re, :] for j in range(nz)]
            vi = [source[phase, j, im, :] for j in range(nz)]
            kr, ki = {}, {}
            reach = [(j - i if conj else i - j) for i in chosen for j in range(nz)]
            for d in sorted(set(reach)):
                kr[d] = k2[base + d, re, :]
                ki[d] = k2[base + d, im, :]
            ks = {d: kr[d] - ki[d] if conj else kr[d] + ki[d] for d in kr}
            vs = [r + i for r, i in zip(vr, vi)]
            for i in chosen:
                a = b = c = None
                for j in range(nz):
                    d = j - i if conj else i - j
                    rr, ii, ss = kr[d] * vr[j], ki[d] * vi[j], ks[d] * vs[j]
                    a = rr if a is None else a + rr
                    b = ii if b is None else b + ii
                    c = ss if c is None else c + ss
                yr = a + b if conj else a - b
                yi = c - a + b if conj else c - a - b
                mix[i, re, :] = mix[i, re, :] + yr if add else yr
                mix[i, im, :] = mix[i, im, :] + yi if add else yi

    def inverse(planes, write, after):
        for z in planes:
            y = jnp.concatenate([mix[z], mix[z + 1]], axis=1)
            hi, lo = split(y)
            both = dot(ix2[...], hi)
            g = both[: 2 * nx] + both[2 * nx :] + dot(ix2[pl.ds(0, 2 * nx), :], lo)
            for k in range(2):
                part = g[:, k * LANES : (k + 1) * LANES]
                rows = jnp.concatenate([part[:nx], part[nx:]], axis=1)
                hi, lo = split(rows)
                write(
                    z + k,
                    dot(hi, iy_hi[...]) + dot(lo, iy_hi[...]) + dot(hi, iy_lo[...]),
                )
            after(z // 2)

    def convolve(phase, field, conj, groups, write, after):
        wait_others(phase, field)
        for q in range(pairs):
            wait_pair(phase, field, q)
            forward(phase, field, q)
        sign = 1 - 2 * gz if conj else 2 * gz - 1
        middle = (extent - 1) // 2
        mix_planes(own, phase, middle, conj, False, range(nz))
        for q in range(pairs):
            swap_copy(phase, q).wait_recv()
        size = nz // groups
        for n in range(groups):
            planes = range(n * size, (n + 1) * size)
            mix_planes(peer, phase, middle + sign * nz, conj, True, planes)
            inverse(planes[::2], write, after)

    zero_missing(0)
    loads[0].wait()
    do_pack(0, est_ref)
    pl.semaphore_wait(barrier, chips)
    for q in range(pairs):
        send_pair(0, est_ref, q)
    send_others(0, est_ref)
    zero_missing(1)

    for load in loads[1:]:
        load.wait()
    chosen = psf[index_ref[0]]
    total = jnp.sum(chosen, axis=0)
    total = jnp.sum(jnp.sum(total, axis=1, keepdims=True), axis=0, keepdims=True)
    psf_pad[...] = jnp.zeros(psf_pad.shape, F32)
    psf_pad[pl.ds(0, extent), pl.ds(0, extent), pl.ds(0, extent)] = chosen * (1.0 / total)[None]
    wide = extent + 1

    @pl.loop(0, wide // 4)
    def _(q):
        block = psf_pad[pl.ds(q * 4, 4)].reshape(4 * wide, LANES)
        hi, lo = split(block)
        x1 = dot(hi, ky_hi[...]) + dot(lo, ky_hi[...]) + dot(hi, ky_lo[...])
        hi, lo = split(x1)
        hi = hi.reshape(4, wide, 2 * LANES)
        lo = lo.reshape(4, wide, 2 * LANES)
        for n, part in enumerate((hi, lo, hi)):
            kd[pl.ds(q * 4, 4), pl.ds(2 * n * wide, wide), :] = part[:, :, :LANES]
            kd[pl.ds(q * 4, 4), pl.ds(2 * n * wide + wide, wide), :] = part[:, :, LANES:]

    @pl.loop(0, wide // 4)
    def _(q):
        for h in range(2):
            n = q * 4 + 2 * h
            pair = jnp.concatenate([kd[n], kd[n + 1]], axis=1)
            spectrum = dot(kx3[...], pair)
            k2[n] = spectrum[:, :LANES]
            k2[n + 1] = spectrum[:, LANES:]

    def write_ratio(z, blurred):
        ratio[z] = view_ref[z] / blurred

    convolve(0, est_ref, False, 2, write_ratio, lambda q: send_pair(1, ratio, q))

    do_pack(1, ratio)
    send_others(1, ratio)

    def write_update(z, correction):
        out_ref[z] = est_ref[z] * correction

    convolve(1, ratio, True, 1, write_update, lambda q: None)

    halves = [(out_ref[2 * i] + out_ref[2 * i + 1]) * 0.5 for i in range(nz // 2)]
    quarters = [(halves[2 * i] + halves[2 * i + 1]) * 0.5 for i in range(nz // 4)]
    eighth = (quarters[0] + quarters[1]) * 0.5

    def pooled(plane):
        hi, lo = split(plane)
        t = dot(hi, py[...]) + dot(lo, py[...])
        hi, lo = split(t)
        return dot(px[...], hi) + dot(px[...], lo)

    r4, c4 = places[3][0], places[3][2]
    last = pooled(eighth)
    share[0] = last[r4 : r4 + 8]
    share_copy = pltpu.make_async_remote_copy(
        src_ref=share.at[0], dst_ref=share_in, send_sem=ps, recv_sem=pr,
        device_id=partner, device_id_type=MESH,
    )
    share_copy.start()
    row, rows, col, cols = places[2]
    three_ref[0] = last[row : row + rows, col : col + cols]
    row, rows, col, cols = places[1]
    for i, plane in enumerate(quarters):
        two_ref[i] = pooled(plane)[row : row + rows, col : col + cols]
    share_copy.wait()
    both = (share[0] + share_in[...]) * 0.5
    four_ref[0] = both[: places[3][1], c4 : c4 + places[3][3]]
    row, rows, col, cols = places[4]
    row = row - r4
    r = lax.broadcasted_iota(jnp.int32, both.shape, 0)
    c = lax.broadcasted_iota(jnp.int32, both.shape, 1)
    inside = (r >= row) & (r < row + rows) & (c >= col) & (c < col + cols)
    mine = jnp.where(inside, both, 0.0)
    height = tiles.shape[1]
    if height > 8:
        mine = jnp.concatenate([mine, jnp.zeros((height - 8, LANES), F32)], axis=0)
    mine = pltpu.roll(mine, lax.rem(gy * cols + LANES - col, LANES), 1)
    mine = pltpu.roll(mine, lax.rem(gx * rows + height - row, height), 0)
    tiles[0] = mine

    def tile_copy(offset):
        return pltpu.make_async_remote_copy(
            src_ref=tiles.at[0], dst_ref=tiles.at[offset],
            send_sem=gs.at[offset], recv_sem=gr.at[offset],
            device_id=chip_at(offset), device_id_type=MESH,
        )

    @pl.loop(1, chips)
    def _(offset):
        tile_copy(offset).start()

    row, rows, col, cols = places[0]
    for i, plane in enumerate(halves):
        one_ref[i] = pooled(plane)[row : row + rows, col : col + cols]
    for phase, field in ((0, est_ref), (1, ratio)):
        wait_sends(phase, field)

    @pl.loop(1, chips)
    def _(offset):
        tile_copy(offset).wait()

    five = tiles[0]
    for offset in range(1, chips):
        five = five + tiles[offset]
    five_ref[0] = five[: five_ref.shape[1], : five_ref.shape[2]]


def write_out(*refs):
    sems = refs[12]
    copies = [pltpu.make_async_copy(refs[i], refs[6 + i], sems.at[i]) for i in range(6)]
    for copy in copies:
        copy.start()
    for copy in copies:
        copy.wait()


def local(sizes, estimate, view_data, psf_stack, view_index):
    gxn, gyn = sizes
    nz, nx, ny = estimate.shape
    views, extent = psf_stack.shape[:2]
    arrays, places = tables(nx, ny, extent)
    lx = nx + 2 * EDGE
    wide = extent + 1
    chips = gxn * gyn
    vmem = pl.BlockSpec(memory_space=pltpu.VMEM)
    hbm = pl.BlockSpec(memory_space=pltpu.HBM)

    def shape(*dims):
        return jax.ShapeDtypeStruct(dims, F32)

    rows5, cols5 = places[4][1] * gxn, places[4][3] * gyn
    dma = pltpu.SemaphoreType.DMA
    shapes = (
        shape(nz, nx, ny),
        shape(nz // 2, nx // 2, ny // 2),
        shape(nz // 4, nx // 4, ny // 4),
        shape(nz // 8, nx // 8, ny // 8),
        shape(1, nx // 16, ny // 16),
        shape(1, rows5, cols5),
    )
    results = pl.pallas_call(
        functools.partial(kernel, sizes, places),
        out_shape=shapes,
        in_specs=[pl.BlockSpec(memory_space=pltpu.SMEM)] + [hbm] * (len(arrays) + 3),
        out_specs=(vmem,) * 6,
        scratch_shapes=[
            pltpu.VMEM((wide, wide, LANES), F32),
            pltpu.VMEM((wide, 6 * wide, LANES), BF),
            pltpu.VMEM((wide, 2 * lx, LANES), F32),
            pltpu.VMEM((2, nz, 2 * lx, LANES), F32),
            pltpu.VMEM((2, nz, 2 * lx, LANES), F32),
            pltpu.VMEM((nz, 2 * lx, LANES), F32),
            pltpu.VMEM((nz, nx, ny), F32),
            pltpu.VMEM((2, 2, nx, LANES), F32),
            pltpu.VMEM((2, 2, nz, EDGE, ny), F32),
            pltpu.VMEM((2, 2, lx, LANES), F32),
            pltpu.VMEM((1, 8, LANES), F32),
            pltpu.VMEM((8, LANES), F32),
            pltpu.VMEM((chips, max(8, rows5), LANES), F32),
            dma((len(arrays) + 3,)),
            dma((2, 2, nz // 2)),
            dma((2, 2, nz // 2)),
            dma((2, 8)),
            dma((2, 8)),
            dma((2, nz // 2)),
            dma((2, nz // 2)),
            dma,
            dma,
            dma((chips,)),
            dma((chips,)),
            *[pltpu.VMEM(a.shape, a.dtype) for a in (estimate, psf_stack, *arrays, view_data)],
        ],
        compiler_params=pltpu.CompilerParams(
            collective_id=0, has_side_effects=True, vmem_limit_bytes=67043328 - 450000
        ),
        name="deconvolve",
    )(view_index, estimate, view_data, psf_stack, *[jnp.asarray(a) for a in arrays])
    return pl.pallas_call(
        write_out,
        out_shape=shapes,
        in_specs=[vmem] * 6,
        out_specs=(hbm,) * 6,
        scratch_shapes=[dma((6,))],
        name="write_out",
    )(*results)


def solution(mesh):
    return jax.shard_map(
        functools.partial(local, (mesh.shape["gx"], mesh.shape["gy"])),
        mesh=mesh,
        in_specs=(P("gz", "gx", "gy"), P("gz", "gx", "gy"), P(), P()),
        out_specs=(
            P("gz", "gx", "gy"),
            P("gz", "gx", "gy"),
            P("gz", "gx", "gy"),
            P("gz", "gx", "gy"),
            P(None, "gx", "gy"),
            P(),
        ),
        check_vma=False,
    )
```
